768 devices in a mesh: dp: 96 (over z, y), mp: 8 (over x, core).
Axes of the slice: x: 4, y: 8, z: 12, core: 2. Of those that a mesh axis runs over, the one named last changes fastest.
Arguments:
- clean: bfloat16 [192, 128, 2432], P('dp'), may hold values from -6 to 6
- noise: bfloat16 [192, 128, 2432], P('dp'), may hold values from -6 to 6
- modulation: float32 [192, 7296], P('dp'), may hold values from -3 to 3
- strata: int32 [192], P('dp'), may hold values from 0 to 63
- up_weight: bfloat16 [2432, 5376], P(None, 'mp'), may hold values from -0.125 to 0.125
- down_weight: bfloat16 [5376, 2432], P('mp'), may hold values from -0.078125 to 0.078125
Outputs:
- up_gradient: float32 [5376, 2432], P(('mp', 'dp'))
- loss_value: float32 [], replicated
The draws below stay inside these ranges and needn't reach their ends.
All inputs are finite; a program needn't handle non-finite values.
Results may differ from the reference program's by a relative error of at most 0.008.
Values may be sent and summed in bfloat16 or wider, within the bound.
No kernel may reach another device: no remote copies, remote signals or barrier semaphores. Data moves between devices by JAX's collectives and lax.ppermute only.
A program may use at most 128 MiB of HBM per device.

```python
import math
import jax
import jax.numpy as jnp
from jax import lax

D = 2432
FFW = 5376
ROWS = 128
STRATA = 64
SAMPLES = 192
N_MP = 8


def draw_strata(key, part):
    middle = STRATA // 2
    positions = jnp.arange(SAMPLES, dtype=jnp.int32)
    base_dist = (SAMPLES - 1 - positions) * (middle - 3) // SAMPLES
    jitter = jax.random.randint(jax.random.fold_in(key, 11), (SAMPLES,), 0, 3, dtype=jnp.int32)
    distance = jnp.minimum(base_dist + jitter, middle - 1)
    side_bit = jax.random.randint(jax.random.fold_in(key, 12), (SAMPLES,), 0, 2, dtype=jnp.int32)
    upper = middle + distance
    lower = middle - 1 - distance
    return jnp.where(side_bit == 1, upper, lower).astype(jnp.int32)


def level_of(key, dims, pieces, smallest, top_value):
    loudness, own = 1.0, jax.random.fold_in(key, 6)
    for position, parts in pieces:
        heights = jnp.exp(jax.random.uniform(jax.random.fold_in(own, position), (parts,), jnp.float32, smallest / len(pieces), top_value / len(pieces)))
        loudness = loudness * jnp.repeat(heights, dims[position] // parts).reshape([-1 if axis == position else 1 for axis in range(len(dims))])
    return loudness


def scatter_about(own_key, extent, deviation, most, shards=(), held_as=jnp.bfloat16):
    factor_of = level_of(own_key, extent, shards, -0.22, 0.18) if shards else 1.0
    array = jax.random.normal(own_key, extent, jnp.float32) * deviation * factor_of
    return jnp.minimum(jnp.maximum(array, -most), most).astype(held_as)


def setup_inputs(seed: int = 0) -> dict:
    splits = jax.random.split(jax.random.key(seed), 7)
    return {
        "clean": scatter_about(splits[0], (SAMPLES, ROWS, D), 1.0, 6.0, ((0, 96),)),
        "noise": scatter_about(splits[1], (SAMPLES, ROWS, D), 1.0, 6.0, ((0, 96),)),
        "modulation": scatter_about(splits[2], (SAMPLES, 3 * D), 0.5, 3.0, ((0, 96),), jnp.float32),
        "strata": draw_strata(jax.random.fold_in(splits[6], 71), 0),
        "up_weight": scatter_about(splits[4], (D, FFW), D ** -0.5, 0.125, ((1, 8),)),
        "down_weight": scatter_about(splits[5], (FFW, D), FFW ** -0.5, 0.078125, ((0, 8),)),
    }


loss_scale = 1048576.0

def stratum_weights(strata):
    quantile = (strata.astype(jnp.float32) + 0.5) / STRATA
    levels = math.sqrt(2.0) * lax.erf_inv(2.0 * quantile - 1.0)
    fraction = jax.nn.sigmoid(levels)
    weight = jnp.exp(-0.5 * levels * levels) / (math.sqrt(2.0 * math.pi) * fraction * (1.0 - fraction))
    return (fraction, weight)

def modulate(clean, noise, modulation, fraction):
    features = clean.shape[-1]
    anchor = clean.astype(jnp.float32)
    drift_field = noise.astype(jnp.float32)
    mix_frac = fraction[:, None, None]
    noisy_field = (1.0 - mix_frac) * anchor + mix_frac * drift_field
    target = drift_field - anchor
    row_mean = lax.optimization_barrier(jnp.mean(noisy_field, -1, keepdims=True))
    centred = noisy_field - row_mean
    variance = lax.optimization_barrier(jnp.mean(centred * centred, -1, keepdims=True))
    normed = centred * lax.rsqrt(variance + 1e-06)
    shifts = modulation[:, None, :features]
    scales = modulation[:, None, features:2 * features]
    modulated = (normed * (1.0 + scales) + shifts).astype(jnp.bfloat16)
    return (noisy_field, target, modulated, modulation[:, 2 * features:])

def gelu_tanh(values):
    return jax.nn.gelu(values, approximate=True)

def reference(clean, noise, modulation, strata, up_weight, down_weight):
    fraction, weight = stratum_weights(strata)
    noisy_field, target, modulated, gate_values = modulate(clean, noise, modulation, fraction)
    flat_rows = modulated.reshape(-1, D)
    shard_cols = FFW // N_MP
    output = jnp.zeros((flat_rows.shape[0], D), jnp.float32)
    for shard_index in range(N_MP):
        lower = shard_index * shard_cols
        preact = jnp.dot(flat_rows, up_weight[:, lower:lower + shard_cols], preferred_element_type=jnp.float32)
        hidden = gelu_tanh(preact).astype(jnp.bfloat16)
        partial_value = jnp.dot(hidden, down_weight[lower:lower + shard_cols], preferred_element_type=jnp.float32).astype(jnp.bfloat16)
        partial_value = lax.optimization_barrier(partial_value)
        output = output + partial_value.astype(jnp.float32)
    predicted = noisy_field + gate_values[:, None, :] * output.reshape(SAMPLES, ROWS, D)
    errors = predicted - target
    weight_sum = jnp.sum(weight)
    row_loss = lax.optimization_barrier(jnp.sum(errors * errors, axis=(1, 2))) / (ROWS * D)
    loss_value = jnp.sum(weight * row_loss) / weight_sum
    coefficient = loss_scale * 2.0 * weight / (weight_sum * ROWS * D)
    slopes = (coefficient[:, None, None] * gate_values[:, None, :] * errors).astype(jnp.bfloat16).reshape(-1, D)
    gradients = []
    for shard_index in range(N_MP):
        lower = shard_index * shard_cols
        preact = jnp.dot(flat_rows, up_weight[:, lower:lower + shard_cols], preferred_element_type=jnp.float32)
        hidden_slope = jnp.dot(slopes, down_weight[lower:lower + shard_cols].T, preferred_element_type=jnp.float32)
        unused, pullback = jax.vjp(gelu_tanh, preact)
        pre_slope = pullback(hidden_slope)[0].astype(jnp.bfloat16)
        gradients.append(jnp.dot(pre_slope.T, flat_rows, preferred_element_type=jnp.float32))
    return (jnp.concatenate(gradients, 0), loss_value)
```

```python
import math

import jax
import jax.numpy as jnp
from jax import lax
from jax.sharding import Mesh
from jax.sharding import PartitionSpec as P

STRATA = 64
DP = ("z", "y")
MP = ("x", "c")
MP_DP = ("x", "c", "z", "y")

loss_scale = 1048576.0


def stratum_weights(strata):
    quantile = (strata.astype(jnp.float32) + 0.5) / STRATA
    levels = math.sqrt(2.0) * lax.erf_inv(2.0 * quantile - 1.0)
    fraction = jax.nn.sigmoid(levels)
    weight = jnp.exp(-0.5 * levels * levels) / (
        math.sqrt(2.0 * math.pi) * fraction * (1.0 - fraction)
    )
    return (fraction, weight)


def blend(clean, noise, fraction):
    anchor = clean.astype(jnp.float32)
    drift_field = noise.astype(jnp.float32)
    noisy_field = (1.0 - fraction) * anchor + fraction * drift_field
    return (noisy_field, drift_field - anchor)


def gelu_tanh(values):
    return jax.nn.gelu(values, approximate=True)


def swap_cores(array):
    return lax.ppermute(array, "c", [(0, 1), (1, 0)])


def exchanged(array, axis):
    return lax.all_to_all(array, axis, 0, 0, tiled=True)


def coded(values):
    first = lax.reduce_precision(values, 8, 7)
    second = lax.reduce_precision(values - first, 8, 7)
    third = (values - first) - second
    return jnp.stack([first, second, third], -1).reshape(-1).astype(jnp.bfloat16)


def decoded(pieces):
    pieces = pieces.astype(jnp.float32)
    return jnp.sum(pieces.reshape(-1, pieces.shape[-1] // 3, 3), axis=(0, 2))


def lane_row(values, lanes):
    return jnp.pad(values, (0, lanes - values.shape[0]))


def with_totals(block, totals):
    row = lane_row(coded(totals), block.shape[-1])
    place = lax.broadcasted_iota(jnp.int32, block.shape, 1)
    return jnp.where(place == block.shape[1] - 1, row, block.astype(jnp.bfloat16))


def local(clean, noise, modulation, strata, up_weight, down_weight):
    samples_here, rows_per, features = clean.shape
    size_x, size_y, size_z = (lax.axis_size(a) for a in ("x", "y", "z"))
    units = up_weight.shape[1]
    share = rows_per // size_x
    core = lax.axis_index("c")
    other_up = swap_cores(up_weight)
    other_down = swap_cores(down_weight)

    def own(array):
        return lax.dynamic_index_in_dim(array, core, 0, keepdims=False)

    fraction, weight = stratum_weights(own(strata))
    latent, drift, conditioning = own(clean), own(noise), own(modulation)
    shift = conditioning[:features]
    scale = conditioning[features : 2 * features]
    gate = conditioning[2 * features :]
    noisy_field, _ = blend(latent, drift, fraction)
    row_mean = jnp.mean(noisy_field, -1, keepdims=True)
    centred = noisy_field - row_mean
    variance = jnp.mean(centred * centred, -1, keepdims=True)
    normed = centred * lax.rsqrt(variance + 1e-06)
    modulated = (normed * (1.0 + scale) + shift).astype(jnp.bfloat16)
    gathered = lax.all_gather(modulated, "y", axis=0, tiled=False)

    ups, downs = (up_weight, other_up), (down_weight, other_down)
    preacts = [jnp.dot(modulated, w, preferred_element_type=jnp.float32) for w in ups]
    partial_value = sum(
        jnp.dot(gelu_tanh(p).astype(jnp.bfloat16), w, preferred_element_type=jnp.float32)
        for p, w in zip(preacts, downs)
    )
    parts = exchanged(partial_value.astype(jnp.bfloat16).reshape(size_x, share, features), "x")
    output = jnp.sum(parts.astype(jnp.float32), axis=0)

    first_row = lax.axis_index("x") * share
    rows = [lax.dynamic_slice_in_dim(a, first_row, share, 0) for a in (latent, drift)]
    noisy_share, target_share = blend(*rows, fraction)
    errors = noisy_share + gate * output - target_share
    loss_local = weight * jnp.sum(errors * errors) / (rows_per * features)
    coefficient = (loss_scale * 2.0 / (rows_per * features)) * weight
    slopes = (coefficient * gate * errors).astype(jnp.bfloat16)
    side = jnp.broadcast_to(lane_row(coded(loss_local), 128), (share, 128))
    message = jnp.concatenate([slopes, side], 1)
    message = exchanged(jnp.broadcast_to(message, (size_x, *message.shape)), "x")
    loss_here = decoded(message[:, 0, features : features + 3])
    slopes = message[:, :, :features].reshape(rows_per, features)

    pre_slopes = []
    for p, w in zip(preacts, downs):
        hidden_slope = lax.dot_general(
            w, slopes, (((1,), (1,)), ((), ())), preferred_element_type=jnp.float32
        )
        unused, pullback = jax.vjp(gelu_tanh, p.T)
        pre_slopes.append(pullback(hidden_slope)[0].astype(jnp.bfloat16))
    group = units // (size_z * size_y)
    pre_slope = jnp.stack(pre_slopes).reshape(2, size_z, size_y, group, rows_per)
    totals = jnp.concatenate([loss_here, weight[None]])
    extra = jnp.broadcast_to(
        lane_row(coded(totals), rows_per), (2, size_z, size_y, 1, rows_per)
    )
    pre_slope = jnp.concatenate([pre_slope, extra], 3).transpose(2, 0, 1, 3, 4)
    pre_slope = exchanged(pre_slope.reshape(size_y, -1, rows_per), "y")
    totals = decoded(pre_slope[:, group, :6])
    gradient = lax.dot_general(
        pre_slope, gathered, (((0, 2), (0, 1)), ((), ())), preferred_element_type=jnp.float32
    ).reshape(2, size_z, group + 1, features)
    received = swap_cores(with_totals(gradient[1], totals))
    totals = totals + decoded(received[0, group, :6])
    gradient = gradient[0] + received.astype(jnp.float32)
    parts = exchanged(with_totals(gradient, totals), "z")
    totals = decoded(parts[:, group, :6])
    gradient = jnp.sum(parts.astype(jnp.float32), axis=0)[:group]
    return (gradient / totals[1], totals[0] / totals[1])


def solution(mesh):
    finer = Mesh(mesh.devices.reshape(12, 8, 4, 2), ("z", "y", "x", "c"))
    return jax.shard_map(
        local,
        mesh=finer,
        in_specs=(
            P(DP, None, None),
            P(DP, None, None),
            P(DP, None),
            P(DP),
            P(None, MP),
            P(MP, None),
        ),
        out_specs=(P(MP_DP, None), P()),
        check_vma=False,
    )
```

```python
import functools
import math

import jax
import jax.numpy as jnp
from jax import lax
from jax.experimental import pallas as pl
from jax.experimental.pallas import tpu as pltpu
from jax.sharding import Mesh
from jax.sharding import PartitionSpec as P


STRATA = 64
DP = ("zb", "zi", "yb", "yi")
MP = ("x", "c")
MP_DP = (*MP, *DP)
LANES = 128
GROUP = 8
VMEM = 56 * 2**20

loss_scale = 1048576.0
f32 = jnp.float32
bf16 = jnp.bfloat16


def swap_cores(array):
    return lax.ppermute(array, "c", [(0, 1), (1, 0)])


def exchanged(array, axis):
    return lax.all_to_all(array, axis, 0, 0, tiled=True)


def gelu_tanh(values):
    return jax.nn.gelu(values, approximate=True)


def gelu_slope(values):
    root = math.sqrt(2.0 / math.pi)
    squares = values * values
    bend = jnp.tanh(root * (values + 0.044715 * squares * values))
    inner = root * (1.0 + (3.0 * 0.044715) * squares)
    return 0.5 * (1.0 + bend) + 0.5 * values * (1.0 - bend * bend) * inner


def erf_inverse(x):
    w = -jnp.log1p(-x * x)
    near = (2.81022636e-08, 3.43273939e-07, -3.5233877e-06, -4.39150654e-06, 0.00021858087,
            -0.00125372503, -0.00417768164, 0.246640727, 1.50140941)
    far = (-0.000200214257, 0.000100950558, 0.00134934322, -0.00367342844, 0.00573950773,
           -0.0076224613, 0.00943887047, 1.00167406, 2.83297682)
    small = w < 5.0
    w = jnp.where(small, w - 2.5, jnp.sqrt(w) - 3.0)
    p = jnp.where(small, near[0], far[0])
    for a, b in zip(near[1:], far[1:]):
        p = jnp.where(small, a, b) + p * w
    return p * x


def coded_row(values):
    lane = lax.broadcasted_iota(jnp.int32, (1, LANES), 1)
    row = jnp.zeros((1, LANES), f32)
    for k, value in enumerate(values):
        first = value.astype(bf16).astype(f32)
        second = (value - first).astype(bf16).astype(f32)
        third = (value - first) - second
        for j, piece in enumerate((first, second, third)):
            row = jnp.where(lane == 3 * k + j, piece, row)
    return row


def decoded(row, k):
    lane = lax.broadcasted_iota(jnp.int32, (1, LANES), 1)
    mine = (lane >= 3 * k) & (lane < 3 * k + 3)
    return jnp.sum(jnp.where(mine, row, 0.0), axis=1, keepdims=True)


def marked(block, row):
    place = lax.broadcasted_iota(jnp.int32, block.shape, 0) % GROUP
    return jnp.where(place == GROUP - 1, row, block)


def blend(clean, noise, fraction):
    anchor = clean.astype(f32)
    drift_field = noise.astype(f32)
    noisy_field = (1.0 - fraction) * anchor + fraction * drift_field
    return (noisy_field, drift_field - anchor)


def modulate_kernel(place, strata, clean, noise, modulation, modulated, info):
    features = clean.shape[-1]
    core = place[0]
    stratum = jnp.full((GROUP, LANES), strata[core].astype(f32), f32)
    level = math.sqrt(2.0) * erf_inverse(2.0 * ((stratum + 0.5) / STRATA) - 1.0)
    fraction = 1.0 / (1.0 + jnp.exp(-level))
    weight = jnp.exp(-0.5 * level * level) / (
        math.sqrt(2.0 * math.pi) * fraction * (1.0 - fraction)
    )
    info[0] = fraction
    info[1] = weight
    noisy_field, _ = blend(clean[0], noise[0], fraction[:1, :1])
    row_mean = jnp.mean(noisy_field, -1, keepdims=True)
    centred = noisy_field - row_mean
    variance = jnp.mean(centred * centred, -1, keepdims=True)
    normed = centred * lax.rsqrt(variance + 1e-06)
    shift = modulation[pl.ds(core, 1), :features]
    scale = modulation[pl.ds(core, 1), features : 2 * features]
    modulated[...] = (normed * (1.0 + scale) + shift).astype(bf16)


def loss_kernel(place, parts, clean, noise, modulation, info, message):
    copies, share, features = parts.shape
    fraction, weight = info[0][:1, :1], info[1][:1, :1]
    gate = modulation[pl.ds(place[0], 1), 2 * features :]
    output = parts[0].astype(f32)
    for j in range(1, copies):
        output = output + parts[j].astype(f32)
    noisy_share, target_share = blend(clean[0], noise[0], fraction)
    errors = noisy_share + gate * output - target_share
    squares = jnp.sum(jnp.sum(errors * errors, axis=0, keepdims=True), axis=1, keepdims=True)
    rows = clean.shape[1] * copies
    loss_local = weight * squares / (rows * features)
    coefficient = (loss_scale * 2.0 / (rows * features)) * weight
    slopes = (coefficient * gate * errors).astype(bf16)
    side = jnp.broadcast_to(coded_row([loss_local]), (share, LANES)).astype(bf16)
    for j in range(copies):
        message[j, :, :features] = slopes
        message[j, :, features:] = side


def backward_kernel(sizes, message, down_0, down_1, pre_0, pre_1, info, out, flat):
    outer_z, inner_z, outer_y, inner_y = sizes
    copies, share, width = message.shape
    features = width - LANES
    units = pre_0.shape[0]
    group = units // math.prod(sizes)
    slopes = message[:, :, :features].reshape(copies * share, features)
    for r, (down, pre) in enumerate(((down_0, pre_0), (down_1, pre_1))):
        hidden_slope = lax.dot_general(
            down[...], slopes, (((1,), (1,)), ((), ())), preferred_element_type=f32
        )
        flat[r * units : (r + 1) * units, :] = gelu_slope(pre[...]) * hidden_slope
    flat[2 * units :, :] = jnp.zeros((GROUP, LANES), f32)
    row = message[0, :1, features:].astype(f32)
    for j in range(1, copies):
        row = row + message[j, :1, features:].astype(f32)
    scalars = coded_row([decoded(row, 0), info[1][:1, :1]])
    for piece in range(inner_z * inner_y):
        zi, yi = divmod(piece, inner_y)
        for at in range(0, 2 * outer_z * outer_y, 2):
            halves = []
            for k in (at, at + 1):
                r, owner = divmod(k, outer_z * outer_y)
                zb, yb = divmod(owner, outer_y)
                owner = ((zb * inner_z + zi) * outer_y + yb) * inner_y + yi
                start = r * units + owner * group
                halves.append(flat[start : start + GROUP, :])
            block = marked(jnp.concatenate(halves, 0), scalars)
            out[piece, at * GROUP : (at + 2) * GROUP, :] = block.astype(bf16)


def gathered_product(place, pre_slope, blocks, first, size):
    columns = [pre_slope[place[2] ^ k, first : first + size, :] for k in range(len(blocks))]
    rows = [block[...] for block in blocks]
    return lax.dot_general(
        jnp.concatenate(columns, 1),
        jnp.concatenate(rows, 0),
        (((1,), (0,)), ((), ())),
        preferred_element_type=f32,
    )


def gathered_sums(pre_slope):
    row = pre_slope[0, :GROUP, :].astype(f32)[GROUP - 1 :, :]
    for k in range(1, pre_slope.shape[0]):
        row = row + pre_slope[k, :GROUP, :].astype(f32)[GROUP - 1 :, :]
    return [decoded(row, k) for k in range(2)]


def store_marked(out, block, sums):
    out[:, LANES:] = block[:, LANES:].astype(bf16)
    out[:, :LANES] = marked(block[:, :LANES], coded_row(sums)).astype(bf16)


def away_kernel(place, pre_slope, *refs):
    *blocks, out = refs
    half = out.shape[0]
    product = gathered_product(place, pre_slope, blocks, half, half)
    store_marked(out, product, gathered_sums(pre_slope))


def home_kernel(place, pre_slope, got, *refs):
    *blocks, out = refs
    half = out.shape[0]
    product = gathered_product(place, pre_slope, blocks, 0, half)
    got_row = got[:GROUP, :LANES].astype(f32)[GROUP - 1 :, :]
    sums = [a + decoded(got_row, k) for k, a in enumerate(gathered_sums(pre_slope))]
    store_marked(out, product + got[...].astype(f32), sums)


def finish_kernel(parts, gradient, loss):
    total = parts[0].astype(f32)
    for j in range(1, parts.shape[0]):
        total = total + parts[j].astype(f32)
    row = total[GROUP - 1 :, :LANES]
    loss_sum, weight_sum = decoded(row, 0), decoded(row, 1)
    gradient[...] = total[: GROUP - 1, :] / weight_sum
    loss[...] = loss_sum / weight_sum


def local(clean, noise, modulation, strata, up_weight, down_weight):
    _, rows_per, features = clean.shape
    sizes = [lax.axis_size(a) for a in ("zb", "zi", "yb", "yi")]
    outer_z, inner_z, outer_y, inner_y = sizes
    size_x = lax.axis_size("x")
    units = up_weight.shape[1]
    share = rows_per // size_x
    shape = jax.ShapeDtypeStruct
    params = pltpu.CompilerParams(vmem_limit_bytes=VMEM)
    call = functools.partial(pl.pallas_call, compiler_params=params)
    other_up = swap_cores(up_weight)
    other_down = swap_cores(down_weight)
    member = lax.axis_index("zi") * inner_y + lax.axis_index("yi")
    place = jnp.stack([lax.axis_index("c"), lax.axis_index("x"), member]).astype(jnp.int32)
    steps = 2
    tile = rows_per // steps
    latent = pl.BlockSpec((1, tile, features), lambda i, place, strata: (place[0], i, 0))
    modulated, info = call(
        modulate_kernel,
        out_shape=(shape((rows_per, features), bf16), shape((2, GROUP, LANES), f32)),
        grid_spec=pltpu.PrefetchScalarGridSpec(
            num_scalar_prefetch=2,
            grid=(steps,),
            in_specs=[
                latent,
                latent,
                pl.BlockSpec(modulation.shape, lambda i, place, strata: (0, 0)),
            ],
            out_specs=[
                pl.BlockSpec((tile, features), lambda i, place, strata: (i, 0)),
                pl.BlockSpec((2, GROUP, LANES), lambda i, place, strata: (0, 0, 0)),
            ],
        ),
        name="modulate",
    )(place, strata, clean, noise, modulation)
    members = inner_z * inner_y
    blocks = [modulated] + [
        lax.ppermute(modulated, ("zi", "yi"), [(i, i ^ k) for i in range(members)])
        for k in range(1, members)
    ]

    ups, downs = (up_weight, other_up), (down_weight, other_down)
    preacts = [jnp.dot(modulated, w, preferred_element_type=f32) for w in ups]
    partial_value = sum(
        jnp.dot(gelu_tanh(p).astype(bf16), w, preferred_element_type=f32)
        for p, w in zip(preacts, downs)
    )
    parts = exchanged(partial_value.astype(bf16).reshape(size_x, share, features), "x")

    share_of = pl.BlockSpec((1, share, features), lambda i, place: (place[0], place[1], 0))
    loss_call = call(
        loss_kernel,
        out_shape=shape((size_x, share, features + LANES), bf16),
        grid_spec=pltpu.PrefetchScalarGridSpec(
            num_scalar_prefetch=1,
            grid=(1,),
            in_specs=[
                pl.BlockSpec(parts.shape, lambda i, place: (0, 0, 0)),
                share_of,
                share_of,
                pl.BlockSpec(modulation.shape, lambda i, place: (0, 0)),
                pl.BlockSpec(info.shape, lambda i, place: (0, 0, 0)),
            ],
            out_specs=pl.BlockSpec(
                (size_x, share, features + LANES), lambda i, place: (0, 0, 0)
            ),
        ),
        name="loss",
    )
    message = loss_call(place, parts, clean, noise, modulation, info)
    message = exchanged(message, "x")

    half = outer_z * outer_y * GROUP
    backward = call(
        functools.partial(backward_kernel, sizes),
        out_shape=shape((members, 2 * half, rows_per), bf16),
        scratch_shapes=[pltpu.VMEM((2 * units + GROUP, rows_per), f32)],
        name="backward",
    )
    pre_slope = backward(message, *downs, *(p.T for p in preacts), info)
    pre_slope = exchanged(pre_slope, ("zi", "yi"))

    whole = pl.BlockSpec(memory_space=pltpu.VMEM)
    scalar = pl.BlockSpec(memory_space=pltpu.SMEM)
    product = functools.partial(call, out_shape=shape((half, features), bf16))
    away = product(away_kernel, in_specs=[scalar] + [whole] * 5, name="away")(
        place, pre_slope, *blocks
    )
    home = product(home_kernel, in_specs=[scalar] + [whole] * 6, name="home")(
        place, pre_slope, swap_cores(away), *blocks
    )
    parts = exchanged(home.reshape(outer_z * outer_y, GROUP, features), ("zb", "yb"))
    gradient, loss = call(
        finish_kernel,
        out_shape=(shape((GROUP - 1, features), f32), shape((1, 1), f32)),
        name="finish",
    )(parts)
    return (gradient, loss[0, 0])


def solution(mesh):
    finer = Mesh(mesh.devices.reshape(6, 2, 4, 2, 4, 2), (*DP, *MP))
    return jax.shard_map(
        local,
        mesh=finer,
        in_specs=(
            P(DP, None, None),
            P(DP, None, None),
            P(DP, None),
            P(DP),
            P(None, MP),
            P(MP, None),
        ),
        out_specs=(P(MP_DP, None), P()),
        check_vma=False,
    )
```

```python
import functools
import math

import jax
import jax.numpy as jnp
from jax import lax
from jax.experimental import pallas as pl
from jax.experimental.pallas import tpu as pltpu
from jax.sharding import Mesh
from jax.sharding import PartitionSpec as P


STRATA = 64
DP = ("zb", "zi", "yb", "yi")
MP = ("x", "c")
MP_DP = (*MP, *DP)
LANES = 128
GROUP = 8
VMEM = 16 * 2**20

loss_scale = 1048576.0
f32 = jnp.float32
bf16 = jnp.bfloat16


def near(*arrays):
    return [pltpu.with_memory_space_constraint(a, pltpu.VMEM) for a in arrays]


def far(*arrays):
    return [pltpu.with_memory_space_constraint(a, pltpu.HBM) for a in arrays]


def swap_cores(array):
    return lax.ppermute(array, "c", [(0, 1), (1, 0)])


def exchanged(array, axis):
    return lax.all_to_all(array, axis, 0, 0, tiled=True)


def gelu_tanh(values):
    return jax.nn.gelu(values, approximate=True)


def gelu_slope(values):
    root = math.sqrt(2.0 / math.pi)
    squares = values * values
    bend = jnp.tanh(root * (values + 0.044715 * squares * values))
    inner = root * (1.0 + (3.0 * 0.044715) * squares)
    return 0.5 * (1.0 + bend) + 0.5 * values * (1.0 - bend * bend) * inner


def erf_inverse(x):
    w = -jnp.log1p(-x * x)
    near = (2.81022636e-08, 3.43273939e-07, -3.5233877e-06, -4.39150654e-06, 0.00021858087,
            -0.00125372503, -0.00417768164, 0.246640727, 1.50140941)
    far = (-0.000200214257, 0.000100950558, 0.00134934322, -0.00367342844, 0.00573950773,
           -0.0076224613, 0.00943887047, 1.00167406, 2.83297682)
    small = w < 5.0
    w = jnp.where(small, w - 2.5, jnp.sqrt(w) - 3.0)
    p = jnp.where(small, near[0], far[0])
    for a, b in zip(near[1:], far[1:]):
        p = jnp.where(small, a, b) + p * w
    return p * x


def coded_row(values):
    lane = lax.broadcasted_iota(jnp.int32, (1, LANES), 1)
    row = jnp.zeros((1, LANES), f32)
    for k, value in enumerate(values):
        first = value.astype(bf16).astype(f32)
        second = (value - first).astype(bf16).astype(f32)
        third = (value - first) - second
        for j, piece in enumerate((first, second, third)):
            row = jnp.where(lane == 3 * k + j, piece, row)
    return row


def decoded(row, k):
    lane = lax.broadcasted_iota(jnp.int32, (1, LANES), 1)
    mine = (lane >= 3 * k) & (lane < 3 * k + 3)
    return jnp.sum(jnp.where(mine, row, 0.0), axis=1, keepdims=True)


def marked(block, row):
    place = lax.broadcasted_iota(jnp.int32, block.shape, 0) % GROUP
    return jnp.where(place == GROUP - 1, row, block)


def blend(clean, noise, fraction):
    anchor = clean.astype(f32)
    drift_field = noise.astype(f32)
    noisy_field = (1.0 - fraction) * anchor + fraction * drift_field
    return (noisy_field, drift_field - anchor)


def modulate_kernel(place, strata, clean, noise, modulation, modulated, info, noisy, target):
    features = clean.shape[-1]
    core = place[0]
    stratum = jnp.full((GROUP, LANES), strata[core].astype(f32), f32)
    level = math.sqrt(2.0) * erf_inverse(2.0 * ((stratum + 0.5) / STRATA) - 1.0)
    fraction = 1.0 / (1.0 + jnp.exp(-level))
    weight = jnp.exp(-0.5 * level * level) / (
        math.sqrt(2.0 * math.pi) * fraction * (1.0 - fraction)
    )
    info[0] = fraction
    info[1] = weight
    noisy_field, _ = blend(clean[0], noise[0], fraction[:1, :1])
    row_mean = jnp.mean(noisy_field, -1, keepdims=True)
    centred = noisy_field - row_mean
    variance = jnp.mean(centred * centred, -1, keepdims=True)
    normed = centred * lax.rsqrt(variance + 1e-06)
    shift = modulation[pl.ds(core, 1), :features]
    scale = modulation[pl.ds(core, 1), features : 2 * features]
    modulated[...] = (normed * (1.0 + scale) + shift).astype(bf16)
    share = noisy.shape[0]
    shares = clean.shape[1] // share

    @pl.when(place[1] // shares == pl.program_id(0))
    def _():
        rows = pl.ds(pl.multiple_of(place[1] % shares * share, share), share)
        noisy[...], target[...] = blend(clean[0, rows, :], noise[0, rows, :], fraction[:1, :1])


def forward_kernel(rows, up_0, up_1, down_0, down_1, out, pre_0, pre_1, *scratch):
    held, arrived = scratch[:3], scratch[3]
    copies = [
        pltpu.make_async_copy(source, place, arrived.at[k])
        for k, (source, place) in enumerate(zip((up_0, up_1, down_0), held))
    ]
    for copy in copies:
        copy.start()
    hidden = []
    for k, pre in enumerate((pre_0, pre_1)):
        copies[k].wait()
        preact = lax.dot_general(
            held[k][...], rows[...], (((1,), (1,)), ((), ())), preferred_element_type=f32
        )
        pre[...] = preact
        hidden.append(gelu_tanh(preact).astype(bf16))
    parts = lax.dot_general(
        hidden[1], down_1[...], (((0,), (0,)), ((), ())), preferred_element_type=f32
    )
    copies[2].wait()
    parts = parts + lax.dot_general(
        hidden[0], held[2][...], (((0,), (0,)), ((), ())), preferred_element_type=f32
    )
    out[...] = parts.astype(bf16)


def loss_kernel(place, parts, noisy, target, modulation, info, message):
    copies, share, features = parts.shape
    weight = info[1][:1, :1]
    gate = modulation[pl.ds(place[0], 1), 2 * features :]
    output = parts[0].astype(f32)
    for j in range(1, copies):
        output = output + parts[j].astype(f32)
    errors = noisy[...] + gate * output - target[...]
    squares = jnp.sum(jnp.sum(errors * errors, axis=0, keepdims=True), axis=1, keepdims=True)
    rows = share * copies
    loss_local = weight * squares / (rows * features)
    coefficient = (loss_scale * 2.0 / (rows * features)) * weight
    slopes = (coefficient * gate * errors).astype(bf16)
    side = jnp.broadcast_to(coded_row([loss_local]), (share, LANES)).astype(bf16)
    for j in range(copies):
        message[j, :, :features] = slopes
        message[j, :, features:] = side


def backward_kernel(sizes, message, down_0, down_1, pre_0, pre_1, info, out, flat):
    outer_z, inner_z, outer_y, inner_y = sizes
    copies, share, width = message.shape
    features = width - LANES
    units = pre_0.shape[0]
    group = units // math.prod(sizes)
    slopes = message[:, :, :features].reshape(copies * share, features)
    for r, (down, pre) in enumerate(((down_0, pre_0), (down_1, pre_1))):
        hidden_slope = lax.dot_general(
            down[...], slopes, (((1,), (1,)), ((), ())), preferred_element_type=f32
        )
        flat[r * units : (r + 1) * units, :] = gelu_slope(pre[...]) * hidden_slope
    flat[2 * units :, :] = jnp.zeros((GROUP, LANES), f32)
    row = message[0, :1, features:].astype(f32)
    for j in range(1, copies):
        row = row + message[j, :1, features:].astype(f32)
    scalars = coded_row([decoded(row, 0), info[1][:1, :1]])
    for piece in range(inner_z * inner_y):
        zi, yi = divmod(piece, inner_y)
        for at in range(0, 2 * outer_z * outer_y, 2):
            halves = []
            for k in (at, at + 1):
                r, owner = divmod(k, outer_z * outer_y)
                yb, zb = divmod(owner, outer_z)
                owner = ((zb * inner_z + zi) * outer_y + yb) * inner_y + yi
                start = r * units + owner * group
                halves.append(flat[start : start + GROUP, :])
            block = marked(jnp.concatenate(halves, 0), scalars)
            out[piece, at * GROUP : (at + 2) * GROUP, :] = block.astype(bf16)


def gathered_product(place, pre_slope, blocks, first, size):
    columns = [pre_slope[place[2] ^ k, first : first + size, :] for k in range(len(blocks))]
    rows = [block[...] for block in blocks]
    return lax.dot_general(
        jnp.concatenate(columns, 1),
        jnp.concatenate(rows, 0),
        (((1,), (0,)), ((), ())),
        preferred_element_type=f32,
    )


def gathered_sums(pre_slope):
    row = pre_slope[0, :GROUP, :].astype(f32)[GROUP - 1 :, :]
    for k in range(1, pre_slope.shape[0]):
        row = row + pre_slope[k, :GROUP, :].astype(f32)[GROUP - 1 :, :]
    return [decoded(row, k) for k in range(2)]


def store_marked(out, block, sums):
    out[:, LANES:] = block[:, LANES:].astype(bf16)
    out[:, :LANES] = marked(block[:, :LANES], coded_row(sums)).astype(bf16)


def away_kernel(place, pre_slope, *refs):
    *blocks, out = refs
    half = out.shape[0]
    product = gathered_product(place, pre_slope, blocks, half, half)
    store_marked(out, product, gathered_sums(pre_slope))


def home_kernel(place, pre_slope, got, *refs):
    *blocks, out, flat = refs
    pieces, rows, _ = out.shape
    half, features = got.shape
    tiles = features // LANES
    kept = GROUP - 1
    product = gathered_product(place, pre_slope, blocks, 0, half)
    got_row = got[:GROUP, :LANES].astype(f32)[GROUP - 1 :, :]
    sums = [a + decoded(got_row, k) for k, a in enumerate(gathered_sums(pre_slope))]
    last = jnp.broadcast_to(coded_row(sums), (rows - kept * tiles, LANES))
    joined = product + got[...].astype(f32)
    for p in range(pieces):
        for t in range(tiles):
            block = joined[p * GROUP : (p + 1) * GROUP, t * LANES : (t + 1) * LANES]
            start = p * rows + t * kept
            flat[start : start + GROUP, :] = block
        flat[p * rows + kept * tiles : (p + 1) * rows, :] = last
        out[p] = flat[p * rows : (p + 1) * rows, :].astype(bf16)


def middle_kernel(kept, parts, out):
    pieces, rows, _ = out.shape
    total = parts[0].astype(f32)
    for j in range(1, parts.shape[0]):
        total = total + parts[j].astype(f32)
    row = total[kept : kept + 1, :]
    scalars = coded_row([decoded(row, k) for k in range(2)])
    place = lax.broadcasted_iota(jnp.int32, (rows, LANES), 0)
    for p in range(pieces):
        block = total[p * rows : (p + 1) * rows, :]
        out[p] = jnp.where(place >= kept, scalars, block).astype(bf16)


def finish_kernel(parts, gradient, loss, flat):
    kept, features = gradient.shape
    tiles = features // LANES
    total = parts[0].astype(f32)
    for j in range(1, parts.shape[0]):
        total = total + parts[j].astype(f32)
    flat[: total.shape[0], :] = total
    row = flat[kept * tiles : kept * tiles + 1, :]
    loss_sum, weight_sum = decoded(row, 0), decoded(row, 1)
    for t in range(tiles):
        block = flat[t * kept : t * kept + GROUP, :]
        gradient[:, t * LANES : (t + 1) * LANES] = (block / weight_sum)[:kept, :]
    loss[...] = loss_sum / weight_sum


def local(clean, noise, modulation, strata, up_weight, down_weight):
    _, rows_per, features = clean.shape
    sizes = [lax.axis_size(a) for a in ("zb", "zi", "yb", "yi")]
    outer_z, inner_z, outer_y, inner_y = sizes
    size_x = lax.axis_size("x")
    units = up_weight.shape[1]
    share = rows_per // size_x
    shape = jax.ShapeDtypeStruct
    params = pltpu.CompilerParams(vmem_limit_bytes=VMEM)
    call = functools.partial(pl.pallas_call, compiler_params=params)
    other_up = swap_cores(up_weight)
    other_down = swap_cores(down_weight)
    member = lax.axis_index("zi") * inner_y + lax.axis_index("yi")
    place = jnp.stack([lax.axis_index("c"), lax.axis_index("x"), member]).astype(jnp.int32)
    steps = 2
    tile = rows_per // steps
    latent = pl.BlockSpec((1, tile, features), lambda i, place, strata: (place[0], i, 0))
    fixed = lambda array: pl.BlockSpec(array.shape, lambda i, *_: (0,) * len(array.shape))
    kept_rows = shape((share, features), f32)
    levels = shape((2, GROUP, LANES), f32)
    modulated, info, noisy, target = call(
        modulate_kernel,
        out_shape=(shape((rows_per, features), bf16), levels, kept_rows, kept_rows),
        grid_spec=pltpu.PrefetchScalarGridSpec(
            num_scalar_prefetch=2,
            grid=(steps,),
            in_specs=[latent, latent, fixed(modulation)],
            out_specs=[
                pl.BlockSpec((tile, features), lambda i, *_: (i, 0)),
                *(fixed(a) for a in (levels, kept_rows, kept_rows)),
            ],
        ),
        name="modulate",
    )(place, *far(strata, clean, noise, modulation))
    members = inner_z * inner_y
    blocks = [modulated] + [
        lax.ppermute(modulated, ("zi", "yi"), [(i, i ^ k) for i in range(members)])
        for k in range(1, members)
    ]

    whole = pl.BlockSpec(memory_space=pltpu.VMEM)
    away_from = pl.BlockSpec(memory_space=pl.ANY)
    ups, downs = (up_weight.T, other_up.T), (down_weight, other_down)
    preact = pltpu.VMEM((units, rows_per), f32)
    forward = call(
        forward_kernel,
        out_shape=(pltpu.VMEM((rows_per, features), bf16), preact, preact),
        in_specs=[whole, away_from, away_from, away_from, whole],
        scratch_shapes=[
            *(pltpu.VMEM((units, features), bf16) for _ in range(3)),
            pltpu.SemaphoreType.DMA((3,)),
        ],
        name="forward",
    )
    partial_value, *preacts = forward(
        modulated, *far(*ups, down_weight), *near(other_down)
    )
    parts = exchanged(partial_value.reshape(size_x, share, features), "x")

    scalar = pl.BlockSpec(memory_space=pltpu.SMEM)
    loss_call = call(
        loss_kernel,
        out_shape=pltpu.VMEM((size_x, share, features + LANES), bf16),
        in_specs=[scalar] + [whole] * 5,
        name="loss",
    )
    message = loss_call(place, *near(parts, noisy, target, modulation, info))
    message = exchanged(message, "x")

    half = outer_z * outer_y * GROUP
    backward = call(
        functools.partial(backward_kernel, sizes),
        out_shape=shape((members, 2 * half, rows_per), bf16),
        in_specs=[whole] * 6,
        scratch_shapes=[pltpu.VMEM((2 * units + GROUP, rows_per), f32)],
        name="backward",
    )
    pre_slope = backward(*near(message, *downs, *preacts, info))
    pre_slope = exchanged(pre_slope, ("zi", "yi"))

    pre_slope, *blocks = near(pre_slope, *blocks)
    away = call(
        away_kernel,
        out_shape=pltpu.VMEM((half, features), bf16),
        in_specs=[scalar] + [whole] * (1 + members),
        name="away",
    )(place, pre_slope, *blocks)
    pieces = outer_z * outer_y
    flat_rows = -(-((GROUP - 1) * features // LANES + 1) // GROUP) * GROUP
    home = call(
        home_kernel,
        out_shape=pltpu.VMEM((pieces, flat_rows, LANES), bf16),
        in_specs=[scalar] + [whole] * (2 + members),
        scratch_shapes=[pltpu.VMEM((pieces * flat_rows, LANES), f32)],
        name="home",
    )(place, pre_slope, *near(swap_cores(away)), *blocks)
    parts = exchanged(home.reshape(outer_y, outer_z * flat_rows, LANES), "yb")
    middle = call(
        functools.partial(middle_kernel, (GROUP - 1) * features // LANES),
        out_shape=pltpu.VMEM((outer_z, flat_rows, LANES), bf16),
        in_specs=[whole],
        name="middle",
    )(*near(parts))
    parts = exchanged(middle, "zb")
    gradient, loss = call(
        finish_kernel,
        out_shape=(shape((GROUP - 1, features), f32), shape((1, 1), f32)),
        in_specs=[whole],
        scratch_shapes=[pltpu.VMEM((flat_rows, LANES), f32)],
        name="finish",
    )(*near(parts))
    return (gradient, loss[0, 0])


def solution(mesh):
    finer = Mesh(mesh.devices.reshape(6, 2, 4, 2, 4, 2), (*DP, *MP))
    return jax.shard_map(
        local,
        mesh=finer,
        in_specs=(
            P(DP, None, None),
            P(DP, None, None),
            P(DP, None),
            P(DP),
            P(None, MP),
            P(MP, None),
        ),
        out_specs=(P(MP_DP, None), P()),
        check_vma=False,
    )
```

```python
import functools
import math

import jax
import jax.numpy as jnp
from jax import lax
from jax.experimental import pallas as pl
from jax.experimental.pallas import tpu as pltpu
from jax.sharding import Mesh
from jax.sharding import PartitionSpec as P


STRATA = 64
DP = ("zb", "zi", "yb", "yi")
MP = ("x", "c")
MP_DP = (*MP, *DP)
LANES = 128
GROUP = 8
VMEM = 16 * 2**20

loss_scale = 1048576.0
f32 = jnp.float32
bf16 = jnp.bfloat16


def near(*arrays):
    return [pltpu.with_memory_space_constraint(a, pltpu.VMEM) for a in arrays]


def far(*arrays):
    return [pltpu.with_memory_space_constraint(a, pltpu.HBM) for a in arrays]


def swap_cores(array):
    return lax.ppermute(array, "c", [(0, 1), (1, 0)])


def exchanged(array, axis):
    return lax.all_to_all(array, axis, 0, 0, tiled=True)


def gelu_tanh(values):
    return jax.nn.gelu(values, approximate=True)


def gelu_slope(values):
    root = math.sqrt(2.0 / math.pi)
    squares = values * values
    bend = jnp.tanh(root * (values + 0.044715 * squares * values))
    inner = root * (1.0 + (3.0 * 0.044715) * squares)
    return 0.5 * (1.0 + bend) + 0.5 * values * (1.0 - bend * bend) * inner


def erf_inverse(x):
    w = -jnp.log1p(-x * x)
    near = (2.81022636e-08, 3.43273939e-07, -3.5233877e-06, -4.39150654e-06, 0.00021858087,
            -0.00125372503, -0.00417768164, 0.246640727, 1.50140941)
    far = (-0.000200214257, 0.000100950558, 0.00134934322, -0.00367342844, 0.00573950773,
           -0.0076224613, 0.00943887047, 1.00167406, 2.83297682)
    small = w < 5.0
    w = jnp.where(small, w - 2.5, jnp.sqrt(w) - 3.0)
    p = jnp.where(small, near[0], far[0])
    for a, b in zip(near[1:], far[1:]):
        p = jnp.where(small, a, b) + p * w
    return p * x


def coded_row(values):
    lane = lax.broadcasted_iota(jnp.int32, (1, LANES), 1)
    row = jnp.zeros((1, LANES), f32)
    for k, value in enumerate(values):
        first = value.astype(bf16).astype(f32)
        second = (value - first).astype(bf16).astype(f32)
        third = (value - first) - second
        for j, piece in enumerate((first, second, third)):
            row = jnp.where(lane == 3 * k + j, piece, row)
    return row


def decoded(row, k):
    lane = lax.broadcasted_iota(jnp.int32, (1, LANES), 1)
    mine = (lane >= 3 * k) & (lane < 3 * k + 3)
    return jnp.sum(jnp.where(mine, row, 0.0), axis=1, keepdims=True)


def marked(block, row):
    place = lax.broadcasted_iota(jnp.int32, block.shape, 0) % GROUP
    return jnp.where(place == GROUP - 1, row, block)


def blend(clean, noise, fraction):
    anchor = clean.astype(f32)
    drift_field = noise.astype(f32)
    noisy_field = (1.0 - fraction) * anchor + fraction * drift_field
    return (noisy_field, drift_field - anchor)


def modulate_kernel(place, strata, clean, noise, modulation, modulated, info, noisy, target):
    features = clean.shape[-1]
    core = place[0]
    stratum = jnp.full((GROUP, LANES), strata[core].astype(f32), f32)
    level = math.sqrt(2.0) * erf_inverse(2.0 * ((stratum + 0.5) / STRATA) - 1.0)
    fraction = 1.0 / (1.0 + jnp.exp(-level))
    weight = jnp.exp(-0.5 * level * level) / (
        math.sqrt(2.0 * math.pi) * fraction * (1.0 - fraction)
    )
    info[0] = fraction
    info[1] = weight
    noisy_field, _ = blend(clean[0], noise[0], fraction[:1, :1])
    row_mean = jnp.mean(noisy_field, -1, keepdims=True)
    centred = noisy_field - row_mean
    variance = jnp.mean(centred * centred, -1, keepdims=True)
    normed = centred * lax.rsqrt(variance + 1e-06)
    shift = modulation[pl.ds(core, 1), :features]
    scale = modulation[pl.ds(core, 1), features : 2 * features]
    modulated[...] = (normed * (1.0 + scale) + shift).astype(bf16)
    share = noisy.shape[0]
    shares = clean.shape[1] // share

    @pl.when(place[1] // shares == pl.program_id(0))
    def _():
        rows = pl.ds(pl.multiple_of(place[1] % shares * share, share), share)
        noisy[...], target[...] = blend(clean[0, rows, :], noise[0, rows, :], fraction[:1, :1])


def forward_kernel(rows, up_0, up_1, down_0, down_1, out, pre_0, pre_1, *scratch):
    held, arrived = scratch[:3], scratch[3]
    copies = [
        pltpu.make_async_copy(source, place, arrived.at[k])
        for k, (source, place) in enumerate(zip((up_0, up_1, down_0), held))
    ]
    for copy in copies:
        copy.start()
    hidden = []
    for k, pre in enumerate((pre_0, pre_1)):
        copies[k].wait()
        preact = lax.dot_general(
            held[k][...], rows[...], (((1,), (1,)), ((), ())), preferred_element_type=f32
        )
        pre[...] = preact
        hidden.append(gelu_tanh(preact).astype(bf16))
    parts = lax.dot_general(
        hidden[1], down_1[...], (((0,), (0,)), ((), ())), preferred_element_type=f32
    )
    copies[2].wait()
    parts = parts + lax.dot_general(
        hidden[0], held[2][...], (((0,), (0,)), ((), ())), preferred_element_type=f32
    )
    out[...] = parts.astype(bf16)


def loss_kernel(place, parts, noisy, target, modulation, info, message):
    copies, share, features = parts.shape
    weight = info[1][:1, :1]
    gate = modulation[pl.ds(place[0], 1), 2 * features :]
    output = parts[0].astype(f32)
    for j in range(1, copies):
        output = output + parts[j].astype(f32)
    errors = noisy[...] + gate * output - target[...]
    squares = jnp.sum(jnp.sum(errors * errors, axis=0, keepdims=True), axis=1, keepdims=True)
    rows = share * copies
    loss_local = weight * squares / (rows * features)
    coefficient = (loss_scale * 2.0 / (rows * features)) * weight
    slopes = (coefficient * gate * errors).astype(bf16)
    side = jnp.broadcast_to(coded_row([loss_local]), (share, LANES)).astype(bf16)
    for j in range(copies):
        message[j, :, :features] = slopes
        message[j, :, features:] = side


def backward_kernel(sizes, message, down_0, down_1, pre_0, pre_1, info, out, flat, held, arrived):
    outer_z, inner_z, outer_y, inner_y = sizes
    copies, share, width = message.shape
    features = width - LANES
    units = pre_0.shape[0]
    group = units // math.prod(sizes)
    fetch = pltpu.make_async_copy(down_1, held, arrived)
    fetch.start()
    slopes = message[:, :, :features].reshape(copies * share, features)
    for r, (down, pre) in enumerate(((down_0, pre_0), (held, pre_1))):
        if r == 1:
            fetch.wait()
        hidden_slope = lax.dot_general(
            down[...], slopes, (((1,), (1,)), ((), ())), preferred_element_type=f32
        )
        flat[r * units : (r + 1) * units, :] = gelu_slope(pre[...]) * hidden_slope
    flat[2 * units :, :] = jnp.zeros((GROUP, LANES), f32)
    row = message[0, :1, features:].astype(f32)
    for j in range(1, copies):
        row = row + message[j, :1, features:].astype(f32)
    scalars = coded_row([decoded(row, 0), info[1][:1, :1]])
    for piece in range(inner_z * inner_y):
        zi, yi = divmod(piece, inner_y)
        for at in range(0, 2 * outer_z * outer_y, 2):
            halves = []
            for k in (at, at + 1):
                r, owner = divmod(k, outer_z * outer_y)
                yb, zb = divmod(owner, outer_z)
                owner = ((zb * inner_z + zi) * outer_y + yb) * inner_y + yi
                start = r * units + owner * group
                halves.append(flat[start : start + GROUP, :])
            block = marked(jnp.concatenate(halves, 0), scalars)
            out[piece, at * GROUP : (at + 2) * GROUP, :] = block.astype(bf16)


def gathered_product(place, pre_slope, blocks, first, size):
    columns = [pre_slope[place[2] ^ k, first : first + size, :] for k in range(len(blocks))]
    rows = [block[...] for block in blocks]
    return lax.dot_general(
        jnp.concatenate(columns, 1),
        jnp.concatenate(rows, 0),
        (((1,), (0,)), ((), ())),
        preferred_element_type=f32,
    )


def gathered_sums(pre_slope):
    row = pre_slope[0, :GROUP, :].astype(f32)[GROUP - 1 :, :]
    for k in range(1, pre_slope.shape[0]):
        row = row + pre_slope[k, :GROUP, :].astype(f32)[GROUP - 1 :, :]
    return [decoded(row, k) for k in range(2)]


def store_marked(out, block, sums):
    out[:, LANES:] = block[:, LANES:].astype(bf16)
    out[:, :LANES] = marked(block[:, :LANES], coded_row(sums)).astype(bf16)


def away_kernel(place, pre_slope, *refs):
    *blocks, out = refs
    half = out.shape[0]
    product = gathered_product(place, pre_slope, blocks, half, half)
    store_marked(out, product, gathered_sums(pre_slope))


def home_kernel(place, pre_slope, got, *refs):
    *blocks, out, flat = refs
    pieces, rows, _ = out.shape
    half, features = got.shape
    tiles = features // LANES
    kept = GROUP - 1
    product = gathered_product(place, pre_slope, blocks, 0, half)
    got_row = got[:GROUP, :LANES].astype(f32)[GROUP - 1 :, :]
    sums = [a + decoded(got_row, k) for k, a in enumerate(gathered_sums(pre_slope))]
    last = jnp.broadcast_to(coded_row(sums), (rows - kept * tiles, LANES))
    joined = product + got[...].astype(f32)
    for p in range(pieces):
        for t in range(tiles):
            block = joined[p * GROUP : (p + 1) * GROUP, t * LANES : (t + 1) * LANES]
            start = p * rows + t * kept
            flat[start : start + GROUP, :] = block
        flat[p * rows + kept * tiles : (p + 1) * rows, :] = last
        out[p] = flat[p * rows : (p + 1) * rows, :].astype(bf16)


def middle_kernel(kept, parts, out):
    pieces, rows, _ = out.shape
    total = parts[0].astype(f32)
    for j in range(1, parts.shape[0]):
        total = total + parts[j].astype(f32)
    row = total[kept : kept + 1, :]
    scalars = coded_row([decoded(row, k) for k in range(2)])
    place = lax.broadcasted_iota(jnp.int32, (rows, LANES), 0)
    for p in range(pieces):
        block = total[p * rows : (p + 1) * rows, :]
        out[p] = jnp.where(place >= kept, scalars, block).astype(bf16)


def finish_kernel(parts, gradient, loss, flat):
    kept, features = gradient.shape
    tiles = features // LANES
    total = parts[0].astype(f32)
    for j in range(1, parts.shape[0]):
        total = total + parts[j].astype(f32)
    flat[: total.shape[0], :] = total
    row = flat[kept * tiles : kept * tiles + 1, :]
    loss_sum, weight_sum = decoded(row, 0), decoded(row, 1)
    for t in range(tiles):
        block = flat[t * kept : t * kept + GROUP, :]
        gradient[:, t * LANES : (t + 1) * LANES] = (block / weight_sum)[:kept, :]
    loss[...] = loss_sum / weight_sum


def local(clean, noise, modulation, strata, up_weight, down_weight):
    _, rows_per, features = clean.shape
    sizes = [lax.axis_size(a) for a in ("zb", "zi", "yb", "yi")]
    outer_z, inner_z, outer_y, inner_y = sizes
    size_x = lax.axis_size("x")
    units = up_weight.shape[1]
    share = rows_per // size_x
    shape = jax.ShapeDtypeStruct
    params = pltpu.CompilerParams(vmem_limit_bytes=VMEM)
    call = functools.partial(pl.pallas_call, compiler_params=params)
    other_up = swap_cores(up_weight)
    other_down = swap_cores(down_weight)
    member = lax.axis_index("zi") * inner_y + lax.axis_index("yi")
    place = jnp.stack([lax.axis_index("c"), lax.axis_index("x"), member]).astype(jnp.int32)
    steps = 2
    tile = rows_per // steps
    latent = pl.BlockSpec((1, tile, features), lambda i, place, strata: (place[0], i, 0))
    fixed = lambda array: pl.BlockSpec(array.shape, lambda i, *_: (0,) * len(array.shape))
    kept_rows = pltpu.HBM((share, features), f32)
    levels = pltpu.HBM((2, GROUP, LANES), f32)
    modulated, info, noisy, target = call(
        modulate_kernel,
        out_shape=(pltpu.HBM((rows_per, features), bf16), levels, kept_rows, kept_rows),
        grid_spec=pltpu.PrefetchScalarGridSpec(
            num_scalar_prefetch=2,
            grid=(steps,),
            in_specs=[latent, latent, fixed(modulation)],
            out_specs=[
                pl.BlockSpec((tile, features), lambda i, *_: (i, 0)),
                *(fixed(a) for a in (levels, kept_rows, kept_rows)),
            ],
        ),
        name="modulate",
    )(place, *far(strata, clean, noise, modulation))
    members = inner_z * inner_y
    blocks = [modulated] + [
        lax.ppermute(modulated, ("zi", "yi"), [(i, i ^ k) for i in range(members)])
        for k in range(1, members)
    ]

    whole = pl.BlockSpec(memory_space=pltpu.VMEM)
    away_from = pl.BlockSpec(memory_space=pl.ANY)
    ups = (up_weight.T, other_up.T)
    preact = pltpu.HBM((units, rows_per), f32)
    forward = pl.pallas_call(
        forward_kernel,
        compiler_params=pltpu.CompilerParams(vmem_limit_bytes=24 * 2**20),
        out_shape=(pltpu.HBM((rows_per, features), bf16), preact, preact),
        in_specs=[whole, away_from, away_from, away_from, whole],
        scratch_shapes=[
            *(pltpu.VMEM((units, features), bf16) for _ in range(3)),
            pltpu.SemaphoreType.DMA((3,)),
        ],
        name="forward",
    )
    partial_value, *preacts = forward(
        *far(modulated, *ups, down_weight), *near(other_down)
    )
    parts = exchanged(partial_value.reshape(size_x, share, features), "x")

    scalar = pl.BlockSpec(memory_space=pltpu.SMEM)
    loss_call = call(
        loss_kernel,
        out_shape=pltpu.VMEM((size_x, share, features + LANES), bf16),
        in_specs=[scalar] + [whole] * 5,
        name="loss",
    )
    message = loss_call(place, *far(parts, noisy, target), *near(modulation, info))
    message = exchanged(message, "x")

    half = outer_z * outer_y * GROUP
    backward = call(
        functools.partial(backward_kernel, sizes),
        out_shape=pltpu.HBM((members, 2 * half, rows_per), bf16),
        in_specs=[whole, whole, away_from, whole, whole, whole],
        scratch_shapes=[
            pltpu.VMEM((2 * units + GROUP, rows_per), f32),
            pltpu.VMEM((units, features), bf16),
            pltpu.SemaphoreType.DMA(()),
        ],
        name="backward",
    )
    pre_slope = backward(
        *near(message, down_weight), *far(other_down), *near(*preacts, info)
    )
    pre_slope = exchanged(pre_slope, ("zi", "yi"))

    pre_slope, *blocks = *near(pre_slope), *far(*blocks)
    away = call(
        away_kernel,
        out_shape=pltpu.VMEM((half, features), bf16),
        in_specs=[scalar] + [whole] * (1 + members),
        name="away",
    )(place, pre_slope, *blocks)
    pieces = outer_z * outer_y
    flat_rows = -(-((GROUP - 1) * features // LANES + 1) // GROUP) * GROUP
    home = call(
        home_kernel,
        out_shape=pltpu.VMEM((pieces, flat_rows, LANES), bf16),
        in_specs=[scalar] + [whole] * (2 + members),
        scratch_shapes=[pltpu.VMEM((pieces * flat_rows, LANES), f32)],
        name="home",
    )(place, pre_slope, *near(swap_cores(away)), *blocks)
    parts = exchanged(home.reshape(outer_y, outer_z * flat_rows, LANES), "yb")
    middle = call(
        functools.partial(middle_kernel, (GROUP - 1) * features // LANES),
        out_shape=pltpu.VMEM((outer_z, flat_rows, LANES), bf16),
        in_specs=[whole],
        name="middle",
    )(*near(parts))
    parts = exchanged(middle, "zb")
    gradient, loss = call(
        finish_kernel,
        out_shape=(shape((GROUP - 1, features), f32), shape((1, 1), f32)),
        in_specs=[whole],
        scratch_shapes=[pltpu.VMEM((flat_rows, LANES), f32)],
        name="finish",
    )(*near(parts))
    return (gradient, loss[0, 0])


def solution(mesh):
    finer = Mesh(mesh.devices.reshape(6, 2, 4, 2, 4, 2), (*DP, *MP))
    return jax.shard_map(
        local,
        mesh=finer,
        in_specs=(
            P(DP, None, None),
            P(DP, None, None),
            P(DP, None),
            P(DP),
            P(None, MP),
            P(MP, None),
        ),
        out_specs=(P(MP_DP, None), P()),
        check_vma=False,
    )
```

```python
import functools
import math

import jax
import jax.numpy as jnp
from jax import lax
from jax.experimental import pallas as pl
from jax.experimental.pallas import tpu as pltpu
from jax.sharding import Mesh
from jax.sharding import PartitionSpec as P


STRATA = 64
DP = ("zb", "zi", "yb", "yi")
MP = ("x", "c")
MP_DP = (*MP, *DP)
LANES = 128
GROUP = 8
VMEM = 16 * 2**20

loss_scale = 1048576.0
f32 = jnp.float32
bf16 = jnp.bfloat16


def near(*arrays):
    return [pltpu.with_memory_space_constraint(a, pltpu.VMEM) for a in arrays]


def far(*arrays):
    return [pltpu.with_memory_space_constraint(a, pltpu.HBM) for a in arrays]


def swap_cores(array):
    return lax.ppermute(array, "c", [(0, 1), (1, 0)])


def exchanged(array, axis):
    return lax.all_to_all(array, axis, 0, 0, tiled=True)


def gelu_tanh(values):
    return jax.nn.gelu(values, approximate=True)


def gelu_slope(values):
    root = math.sqrt(2.0 / math.pi)
    squares = values * values
    bend = jnp.tanh(root * (values + 0.044715 * squares * values))
    inner = root * (1.0 + (3.0 * 0.044715) * squares)
    return 0.5 * (1.0 + bend) + 0.5 * values * (1.0 - bend * bend) * inner


def erf_inverse(x):
    w = -jnp.log1p(-x * x)
    near = (2.81022636e-08, 3.43273939e-07, -3.5233877e-06, -4.39150654e-06, 0.00021858087,
            -0.00125372503, -0.00417768164, 0.246640727, 1.50140941)
    far = (-0.000200214257, 0.000100950558, 0.00134934322, -0.00367342844, 0.00573950773,
           -0.0076224613, 0.00943887047, 1.00167406, 2.83297682)
    small = w < 5.0
    w = jnp.where(small, w - 2.5, jnp.sqrt(w) - 3.0)
    p = jnp.where(small, near[0], far[0])
    for a, b in zip(near[1:], far[1:]):
        p = jnp.where(small, a, b) + p * w
    return p * x


def coded_row(values):
    lane = lax.broadcasted_iota(jnp.int32, (1, LANES), 1)
    row = jnp.zeros((1, LANES), f32)
    for k, value in enumerate(values):
        first = value.astype(bf16).astype(f32)
        second = (value - first).astype(bf16).astype(f32)
        third = (value - first) - second
        for j, piece in enumerate((first, second, third)):
            row = jnp.where(lane == 3 * k + j, piece, row)
    return row


def decoded(row, k):
    lane = lax.broadcasted_iota(jnp.int32, (1, LANES), 1)
    mine = (lane >= 3 * k) & (lane < 3 * k + 3)
    return jnp.sum(jnp.where(mine, row, 0.0), axis=1, keepdims=True)


def marked(block, row):
    place = lax.broadcasted_iota(jnp.int32, block.shape, 0) % GROUP
    return jnp.where(place == GROUP - 1, row, block)


def blend(clean, noise, fraction):
    anchor = clean.astype(f32)
    drift_field = noise.astype(f32)
    noisy_field = (1.0 - fraction) * anchor + fraction * drift_field
    return (noisy_field, drift_field - anchor)


def modulate_kernel(place, strata, clean, noise, modulation, up, *rest):
    modulated, info, noisy, target, up_near, rows_near, arrived = rest
    features = clean.shape[-1]
    fetch = pltpu.make_async_copy(up, up_near, arrived)

    @pl.when(pl.program_id(0) == 0)
    def _():
        fetch.start()

    core = place[0]
    stratum = jnp.full((GROUP, LANES), strata[core].astype(f32), f32)
    level = math.sqrt(2.0) * erf_inverse(2.0 * ((stratum + 0.5) / STRATA) - 1.0)
    fraction = 1.0 / (1.0 + jnp.exp(-level))
    weight = jnp.exp(-0.5 * level * level) / (
        math.sqrt(2.0 * math.pi) * fraction * (1.0 - fraction)
    )
    info[0] = fraction
    info[1] = weight
    noisy_field, _ = blend(clean[0], noise[0], fraction[:1, :1])
    row_mean = jnp.mean(noisy_field, -1, keepdims=True)
    centred = noisy_field - row_mean
    variance = jnp.mean(centred * centred, -1, keepdims=True)
    normed = centred * lax.rsqrt(variance + 1e-06)
    shift = modulation[pl.ds(core, 1), :features]
    scale = modulation[pl.ds(core, 1), features : 2 * features]
    tile = clean.shape[1]
    at = pl.ds(pl.multiple_of(pl.program_id(0) * tile, tile), tile)
    rows_here = (normed * (1.0 + scale) + shift).astype(bf16)
    modulated[...] = rows_here
    rows_near[at, :] = rows_here
    share = noisy.shape[0]
    shares = clean.shape[1] // share

    @pl.when(place[1] // shares == pl.program_id(0))
    def _():
        rows = pl.ds(pl.multiple_of(place[1] % shares * share, share), share)
        noisy[...], target[...] = blend(clean[0, rows, :], noise[0, rows, :], fraction[:1, :1])

    @pl.when(pl.program_id(0) == pl.num_programs(0) - 1)
    def _():
        fetch.wait()


def loss_kernel(place, parts, noisy, target, modulation, info, message):
    copies, share, features = parts.shape
    weight = info[1][:1, :1]
    gate = modulation[pl.ds(place[0], 1), 2 * features :]
    output = parts[0].astype(f32)
    for j in range(1, copies):
        output = output + parts[j].astype(f32)
    errors = noisy[...] + gate * output - target[...]
    squares = jnp.sum(jnp.sum(errors * errors, axis=0, keepdims=True), axis=1, keepdims=True)
    rows = share * copies
    loss_local = weight * squares / (rows * features)
    coefficient = (loss_scale * 2.0 / (rows * features)) * weight
    slopes = (coefficient * gate * errors).astype(bf16)
    side = jnp.broadcast_to(coded_row([loss_local]), (share, LANES)).astype(bf16)
    for j in range(copies):
        message[j, :, :features] = slopes
        message[j, :, features:] = side


def backward_kernel(sizes, message, down_0, down_1, pre_0, pre_1, info, out, flat):
    outer_z, inner_z, outer_y, inner_y = sizes
    copies, share, width = message.shape
    features = width - LANES
    units = pre_0.shape[0]
    group = units // math.prod(sizes)
    slopes = message[:, :, :features].reshape(copies * share, features)
    for r, (down, pre) in enumerate(((down_0, pre_0), (down_1, pre_1))):
        hidden_slope = lax.dot_general(
            down[...], slopes, (((1,), (1,)), ((), ())), preferred_element_type=f32
        )
        flat[r * units : (r + 1) * units, :] = gelu_slope(pre[...]) * hidden_slope
    flat[2 * units :, :] = jnp.zeros((GROUP, LANES), f32)
    row = message[0, :1, features:].astype(f32)
    for j in range(1, copies):
        row = row + message[j, :1, features:].astype(f32)
    scalars = coded_row([decoded(row, 0), info[1][:1, :1]])
    for piece in range(inner_z * inner_y):
        zi, yi = divmod(piece, inner_y)
        for at in range(0, 2 * outer_z * outer_y, 2):
            halves = []
            for k in (at, at + 1):
                r, owner = divmod(k, outer_z * outer_y)
                yb, zb = divmod(owner, outer_z)
                owner = ((zb * inner_z + zi) * outer_y + yb) * inner_y + yi
                start = r * units + owner * group
                halves.append(flat[start : start + GROUP, :])
            block = marked(jnp.concatenate(halves, 0), scalars)
            out[piece, at * GROUP : (at + 2) * GROUP, :] = block.astype(bf16)


def gathered_product(place, pre_slope, blocks, first, size):
    columns = [pre_slope[place[2] ^ k, first : first + size, :] for k in range(len(blocks))]
    rows = [block[...] for block in blocks]
    return lax.dot_general(
        jnp.concatenate(columns, 1),
        jnp.concatenate(rows, 0),
        (((1,), (0,)), ((), ())),
        preferred_element_type=f32,
    )


def gathered_sums(pre_slope):
    row = pre_slope[0, :GROUP, :].astype(f32)[GROUP - 1 :, :]
    for k in range(1, pre_slope.shape[0]):
        row = row + pre_slope[k, :GROUP, :].astype(f32)[GROUP - 1 :, :]
    return [decoded(row, k) for k in range(2)]


def store_marked(out, block, sums):
    out[:, LANES:] = block[:, LANES:].astype(bf16)
    out[:, :LANES] = marked(block[:, :LANES], coded_row(sums)).astype(bf16)


def away_kernel(place, pre_slope, *refs):
    *blocks, out = refs
    half = out.shape[0]
    product = gathered_product(place, pre_slope, blocks, half, half)
    store_marked(out, product, gathered_sums(pre_slope))


def home_kernel(place, pre_slope, got, *refs):
    *blocks, out, flat = refs
    pieces, rows, _ = out.shape
    half, features = got.shape
    tiles = features // LANES
    kept = GROUP - 1
    product = gathered_product(place, pre_slope, blocks, 0, half)
    got_row = got[:GROUP, :LANES].astype(f32)[GROUP - 1 :, :]
    sums = [a + decoded(got_row, k) for k, a in enumerate(gathered_sums(pre_slope))]
    last = jnp.broadcast_to(coded_row(sums), (rows - kept * tiles, LANES))
    joined = product + got[...].astype(f32)
    for p in range(pieces):
        for t in range(tiles):
            block = joined[p * GROUP : (p + 1) * GROUP, t * LANES : (t + 1) * LANES]
            start = p * rows + t * kept
            flat[start : start + GROUP, :] = block
        flat[p * rows + kept * tiles : (p + 1) * rows, :] = last
        out[p] = flat[p * rows : (p + 1) * rows, :].astype(bf16)


def middle_kernel(kept, parts, out):
    pieces, rows, _ = out.shape
    total = parts[0].astype(f32)
    for j in range(1, parts.shape[0]):
        total = total + parts[j].astype(f32)
    row = total[kept : kept + 1, :]
    scalars = coded_row([decoded(row, k) for k in range(2)])
    place = lax.broadcasted_iota(jnp.int32, (rows, LANES), 0)
    for p in range(pieces):
        block = total[p * rows : (p + 1) * rows, :]
        out[p] = jnp.where(place >= kept, scalars, block).astype(bf16)


def finish_kernel(parts, gradient, loss, flat):
    kept, features = gradient.shape
    tiles = features // LANES
    total = parts[0].astype(f32)
    for j in range(1, parts.shape[0]):
        total = total + parts[j].astype(f32)
    flat[: total.shape[0], :] = total
    row = flat[kept * tiles : kept * tiles + 1, :]
    loss_sum, weight_sum = decoded(row, 0), decoded(row, 1)
    for t in range(tiles):
        block = flat[t * kept : t * kept + GROUP, :]
        gradient[:, t * LANES : (t + 1) * LANES] = (block / weight_sum)[:kept, :]
    loss[...] = loss_sum / weight_sum


def local(clean, noise, modulation, strata, up_weight, down_weight):
    _, rows_per, features = clean.shape
    sizes = [lax.axis_size(a) for a in ("zb", "zi", "yb", "yi")]
    outer_z, inner_z, outer_y, inner_y = sizes
    size_x = lax.axis_size("x")
    units = up_weight.shape[1]
    share = rows_per // size_x
    shape = jax.ShapeDtypeStruct
    params = pltpu.CompilerParams(vmem_limit_bytes=VMEM)
    call = functools.partial(pl.pallas_call, compiler_params=params)
    other_down = swap_cores(down_weight)
    other_up = swap_cores(up_weight.T).T

    member = lax.axis_index("zi") * inner_y + lax.axis_index("yi")
    place = jnp.stack([lax.axis_index("c"), lax.axis_index("x"), member]).astype(jnp.int32)
    whole = pl.BlockSpec(memory_space=pltpu.VMEM)
    steps = 2
    tile = rows_per // steps
    latent = pl.BlockSpec((1, tile, features), lambda i, place, strata: (place[0], i, 0))
    fixed = lambda array: pl.BlockSpec(array.shape, lambda i, *_: (0,) * len(array.shape))
    kept_rows = shape((share, features), f32)
    levels = shape((2, GROUP, LANES), f32)
    modulated, info, noisy, target, up_near, rows_near = call(
        modulate_kernel,
        out_shape=(
            shape((rows_per, features), bf16),
            levels,
            kept_rows,
            kept_rows,
            pltpu.VMEM((units, features), bf16),
            pltpu.VMEM((rows_per, features), bf16),
        ),
        grid_spec=pltpu.PrefetchScalarGridSpec(
            num_scalar_prefetch=2,
            grid=(steps,),
            in_specs=[latent, latent, fixed(modulation), pl.BlockSpec(memory_space=pl.ANY)],
            out_specs=[
                pl.BlockSpec((tile, features), lambda i, *_: (i, 0)),
                *(fixed(a) for a in (levels, kept_rows, kept_rows)),
                whole,
                whole,
            ],
            scratch_shapes=[pltpu.SemaphoreType.DMA(())],
        ),
        name="modulate",
    )(place, *far(strata, clean, noise, modulation, up_weight.T))
    members = inner_z * inner_y
    blocks = [modulated] + [
        lax.ppermute(modulated, ("zi", "yi"), [(i, i ^ k) for i in range(members)])
        for k in range(1, members)
    ]

    ups, downs = (up_near.T, other_up), (down_weight, other_down)
    preacts = [jnp.dot(rows_near, w, preferred_element_type=f32) for w in ups]
    partial_value = sum(
        jnp.dot(gelu_tanh(p).astype(bf16), w, preferred_element_type=f32)
        for p, w in zip(preacts, downs)
    )
    parts = exchanged(partial_value.astype(bf16).reshape(size_x, share, features), "x")

    scalar = pl.BlockSpec(memory_space=pltpu.SMEM)
    loss_call = call(
        loss_kernel,
        out_shape=pltpu.VMEM((size_x, share, features + LANES), bf16),
        in_specs=[scalar] + [whole] * 5,
        name="loss",
    )
    message = loss_call(place, *near(parts, noisy, target, modulation, info))
    message = exchanged(message, "x")

    half = outer_z * outer_y * GROUP
    backward = call(
        functools.partial(backward_kernel, sizes),
        out_shape=shape((members, 2 * half, rows_per), bf16),
        in_specs=[whole] * 6,
        scratch_shapes=[pltpu.VMEM((2 * units + GROUP, rows_per), f32)],
        name="backward",
    )
    pre_slope = backward(*near(message, *downs, *(p.T for p in preacts), info))
    pre_slope = exchanged(pre_slope, ("zi", "yi"))

    pre_slope, *blocks = near(pre_slope, *blocks)
    away = call(
        away_kernel,
        out_shape=pltpu.VMEM((half, features), bf16),
        in_specs=[scalar] + [whole] * (1 + members),
        name="away",
    )(place, pre_slope, *blocks)
    pieces = outer_z * outer_y
    flat_rows = -(-((GROUP - 1) * features // LANES + 1) // GROUP) * GROUP
    home = call(
        home_kernel,
        out_shape=pltpu.VMEM((pieces, flat_rows, LANES), bf16),
        in_specs=[scalar] + [whole] * (2 + members),
        scratch_shapes=[pltpu.VMEM((pieces * flat_rows, LANES), f32)],
        name="home",
    )(place, pre_slope, *near(swap_cores(away)), *blocks)
    parts = exchanged(home.reshape(outer_y, outer_z * flat_rows, LANES), "yb")
    middle = call(
        functools.partial(middle_kernel, (GROUP - 1) * features // LANES),
        out_shape=pltpu.VMEM((outer_z, flat_rows, LANES), bf16),
        in_specs=[whole],
        name="middle",
    )(*near(parts))
    parts = exchanged(middle, "zb")
    gradient, loss = call(
        finish_kernel,
        out_shape=(shape((GROUP - 1, features), f32), shape((1, 1), f32)),
        in_specs=[whole],
        scratch_shapes=[pltpu.VMEM((flat_rows, LANES), f32)],
        name="finish",
    )(*near(parts))
    return (gradient, loss[0, 0])


def solution(mesh):
    finer = Mesh(mesh.devices.reshape(6, 2, 4, 2, 4, 2), (*DP, *MP))
    return jax.shard_map(
        local,
        mesh=finer,
        in_specs=(
            P(DP, None, None),
            P(DP, None, None),
            P(DP, None),
            P(DP),
            P(None, MP),
            P(MP, None),
        ),
        out_specs=(P(MP_DP, None), P()),
        check_vma=False,
    )
```
